32 devices in a mesh: data: 4 (over y, z), tp: 8 (over x, core).
Axes of the slice: x: 4, y: 2, z: 2, core: 2. Of those that a mesh axis runs over, the one named last changes fastest.
The devices are a block of a 4x4x8 slice.
Arguments:
- x: bfloat16 [16384, 14336], P('data', 'tp'), parts along dimension 0
- w: bfloat16 [14336, 4096], P('tp')
- r: bfloat16 [16384, 4096], P('data'), parts along dimension 0
- g: bfloat16 [4096], replicated
Outputs:
- output: bfloat16 [16384, 4096], P('data'), parts along dimension 0
There are 4 independent parts. The reference program is written for one: setup_inputs(seed, part) draws one part's arguments, and reference() takes and returns one part's arrays. A program takes and returns all parts, laid end to end along the dimension named above; an argument that names none is the same for every part.
All inputs are finite; a program needn't handle non-finite values.
Results may differ from the reference program's by a relative error of at most 0.0108178.
Values are sent between devices in bfloat16 or wider.
A program may use at most 768 MiB of HBM per device.

```python
import jax
import jax.numpy as jnp
from jax import lax

T = 4096
H = 4096
F = 14336
EPS = 1e-6


def setup_inputs(seed: int = 0, part: int = 0) -> dict:
    kp = jax.random.fold_in(jax.random.key(seed), part)
    kx, kr = jax.random.split(kp)
    kw, kg = jax.random.split(jax.random.key(seed + 1))
    x = jax.random.normal(kx, (T, F), jnp.float32).astype(jnp.bfloat16)
    w = (jax.random.normal(kw, (F, H), jnp.float32) * (F ** -0.5)).astype(jnp.bfloat16)
    r = jax.random.normal(kr, (T, H), jnp.float32).astype(jnp.bfloat16)
    g = jax.random.uniform(kg, (H,), jnp.float32, 0.5, 1.5).astype(jnp.bfloat16)
    return {"x": x, "w": w, "r": r, "g": g}


def reference(x, w, r, g):
    y = jnp.dot(x, w, preferred_element_type=jnp.float32).astype(jnp.bfloat16)
    a = r.astype(jnp.float32) + y.astype(jnp.float32)
    ms = jnp.mean(a * a, axis=-1, keepdims=True)
    z = a * lax.rsqrt(ms + EPS) * g.astype(jnp.float32)
    return z.astype(jnp.bfloat16)
```

```python
import functools

import jax
import jax.numpy as jnp
from jax import lax
from jax.experimental import pallas as pl
from jax.experimental.pallas import tpu as pltpu
from jax.sharding import PartitionSpec as P

EPS = 1e-6
MESH = pl.DeviceIdType.MESH
NC = 4
NS = 4


def kernel(
    tp, x, w, r, g, out,
    xbuf, wbuf, gbuf, rbuf, stage, part, recv,
    x_sem, w_sem, g_sem, pair_s, pair_r, rs_s, rs_r, cb_s, cb_r,
    ag_s, ag_r, fw_s, fw_r, sib_s, sib_r, loc_s,
):
    n = tp // 2
    blk = part.shape[1]
    cols = wbuf.shape[2]
    sub = blk // NS
    me = lax.axis_index("tp")
    chip = me // 2
    core = me - 2 * chip
    sib = 2 * chip + 1 - core

    def chip_at(d):
        return lax.rem(chip + d + n, n)

    right = 2 * chip_at(1) + core
    left = 2 * chip_at(-1) + core

    def row_of(q, k, o):
        return pl.multiple_of(blk * (4 * q + 2 * k + o), blk)

    def remote(src, dst, ss, rs, dev):
        return pltpu.make_async_remote_copy(
            src_ref=src, dst_ref=dst, send_sem=ss, recv_sem=rs,
            device_id={"tp": dev}, device_id_type=MESH,
        )

    def load_x(pair):
        res = []
        for side in range(2):
            sign = 1 - 2 * side
            q = chip_at(sign * ((4 - pair) // 2))
            o = lax.rem(side + 1 + pair, 2)
            for which in range(2):
                k = core if which == 0 else 1 - core
                slot = lax.rem(pair, 2)
                res.append(pltpu.make_async_copy(
                    x.at[pl.ds(row_of(q, k, o), blk), :],
                    xbuf.at[slot, 2 * side + which],
                    x_sem.at[slot, 2 * side + which],
                ))
        return res

    def load_w(c):
        return pltpu.make_async_copy(
            w.at[:, pl.ds(pl.multiple_of(c * cols, cols), cols)], wbuf.at[c], w_sem.at[c]
        )

    def col(c):
        return pl.ds(pl.multiple_of(c * cols, cols), cols)

    def row(s):
        return pl.ds(pl.multiple_of(s * sub, sub), sub)

    for cp in load_x(0):
        cp.start()
    for c in range(NC):
        load_w(c).start()
    for cp in load_x(1):
        cp.start()
    own0 = row_of(chip, core, 0)
    load_r = pltpu.make_async_copy(r.at[pl.ds(own0, 2 * blk), :], rbuf, g_sem.at[0])
    load_g = pltpu.make_async_copy(g, gbuf, g_sem.at[1])
    load_r.start()
    load_g.start()

    barrier = pltpu.get_barrier_semaphore()
    for dev in (sib, left, right):
        pl.semaphore_signal(barrier, inc=1, device_id={"tp": dev}, device_id_type=MESH)
    pl.semaphore_wait(barrier, 3)

    per = 2 * NC
    steps = 4 * per

    def split(t):
        pair = t // per
        c = (t - pair * per) // 2
        side = t - 2 * (t // 2)
        return pair, c, side

    def pair_copy(t):
        pair, c, side = split(t)
        return remote(
            stage.at[lax.rem(t, 4)], part.at[2 * pair + side, :, col(c)],
            pair_s.at[lax.rem(t, 4)], pair_r.at[t], sib,
        )

    def rs_copy(t):
        pair, c, side = split(t)
        job = 2 * pair + side
        return remote(
            part.at[job, :, col(c)], recv.at[job, :, col(c)],
            rs_s.at[t], rs_r.at[t], jnp.where(side == 0, right, left),
        )

    def product(pair, side, which, c):
        return jnp.dot(
            xbuf[lax.rem(pair, 2), 2 * side + which], wbuf[c],
            preferred_element_type=jnp.float32,
        )

    @pl.loop(0, steps + 1)
    def _(t):
        @pl.when(t < steps)
        def _():
            pair, c, side = split(t)

            @pl.when(lax.rem(t, per) == 0)
            def _():
                for cp in load_x(pair):
                    cp.wait()

            @pl.when(jnp.logical_and(t < per, side == 0))
            def _():
                load_w(c).wait()

            @pl.when(t >= 4)
            def _():
                pair_copy(t - 4).wait_send()

            stage[lax.rem(t, 4)] = product(pair, side, 1, c).astype(jnp.bfloat16)
            pair_copy(t).start()

        @pl.when(t > 0)
        def _():
            u = t - 1
            pair, c, side = split(u)
            job = 2 * pair + side
            pair_copy(u).wait_recv()
            acc = product(pair, side, 0, c)
            acc = acc + part[job, :, col(c)].astype(jnp.float32)
            part[job, :, col(c)] = acc.astype(jnp.bfloat16)

            @pl.when(u < 2 * per)
            def _():
                rs_copy(u).start()

            @pl.when(jnp.logical_and(lax.rem(u, per) == per - 1, pair < 2))
            def _():
                for cp in load_x(pair + 2):
                    cp.start()

    def cb_copy(i):
        s = i // 2
        side = i - 2 * s
        return remote(
            part.at[4 + side, row(s), :], recv.at[4 + side, row(s), :],
            cb_s.at[i], cb_r.at[i], jnp.where(side == 0, right, left),
        )

    @pl.loop(0, per)
    def _(t):
        rs_copy(t).wait_recv()

    @pl.loop(0, 2 * NS)
    def _(i):
        s = i // 2
        side = i - 2 * s
        total = part[4 + side, row(s), :].astype(jnp.float32)
        total = total + recv[side, row(s), :].astype(jnp.float32)
        part[4 + side, row(s), :] = total.astype(jnp.bfloat16)
        cb_copy(i).start()

    @pl.loop(per, 2 * per)
    def _(t):
        rs_copy(t).wait_recv()

    load_r.wait()
    load_g.wait()

    def out_rows(q, o, s, k=None):
        k = core if k is None else k
        return out.at[pl.ds(pl.multiple_of(row_of(q, k, o) + s * sub, sub), sub), :]

    def ag_copy(i, d):
        s = i // 2
        o = i - 2 * s
        return remote(
            part.at[6 + o, row(s), :], out_rows(chip, o, s),
            ag_s.at[d, i], ag_r.at[d, i], right if d == 0 else left,
        )

    def own_sib(i):
        s = i // 2
        o = i - 2 * s
        return remote(
            part.at[6 + o, row(s), :], out_rows(chip, o, s),
            sib_s.at[0, i], sib_r.at[0, i], sib,
        )

    def own_out(i):
        s = i // 2
        o = i - 2 * s
        return pltpu.make_async_copy(part.at[6 + o, row(s), :], out_rows(chip, o, s), loc_s.at[i])

    grp = 16 if sub % 16 == 0 else sub

    @pl.loop(0, 2 * NS)
    def _(i):
        s = i // 2
        o = i - 2 * s
        cb_copy(2 * s + 1 - o).wait_recv()

        @pl.loop(0, sub // grp)
        def _(b):
            rows = pl.ds(pl.multiple_of(s * sub + b * grp, grp), grp)
            y = part[6 + o, rows, :].astype(jnp.float32)
            y = y + recv[2 + o, rows, :].astype(jnp.float32)
            y = y + recv[5 - o, rows, :].astype(jnp.float32)
            rr = rbuf[pl.ds(pl.multiple_of(o * blk + s * sub + b * grp, grp), grp), :]
            a = rr.astype(jnp.float32) + y.astype(jnp.bfloat16).astype(jnp.float32)
            ms = jnp.mean(a * a, axis=-1, keepdims=True)
            z = a * lax.rsqrt(ms + EPS) * gbuf[...].astype(jnp.float32)
            part[6 + o, rows, :] = z.astype(jnp.bfloat16)

        ag_copy(i, 0).start()
        ag_copy(i, 1).start()
        own_sib(i).start()
        own_out(i).start()

    def sib_copy(d, i):
        s = i // 2
        o = i - 2 * s
        rows = out_rows(chip_at(-1 if d == 0 else 1), o, s)
        return remote(rows, rows, sib_s.at[1 + d, i], sib_r.at[1 + d, i], sib)

    def fw_copy(d, s):
        rows = out_rows(chip_at(-1 if d == 0 else 1), d, s)
        return remote(rows, rows, fw_s.at[d, s], fw_r.at[d, s], right if d == 0 else left)

    def fw_sib(d, s):
        rows = out_rows(chip_at(2), d, s)
        return remote(rows, rows, sib_s.at[3, 2 * s + d], sib_r.at[3, 2 * s + d], sib)

    @pl.loop(0, NS)
    def _(s):
        for o in range(2):
            i = 2 * s + o
            for d in range(2):
                ag_copy(i, d).wait_recv()
                if o == d:
                    fw_copy(d, s).start()
                sib_copy(d, i).start()

    @pl.loop(0, NS)
    def _(s):
        for d in range(2):
            rows = out_rows(chip_at(2), d, s)
            remote(rows, rows, fw_s.at[d, s], fw_r.at[d, s], sib).wait_recv()
            fw_sib(d, s).start()

    @pl.loop(steps - 4, steps)
    def _(t):
        pair_copy(t).wait_send()

    @pl.loop(0, 2 * per)
    def _(t):
        rs_copy(t).wait_send()

    @pl.loop(0, 2 * NS)
    def _(i):
        cb_copy(i).wait_send()
        own_out(i).wait()
        own_sib(i).wait()
        for d in range(2):
            ag_copy(i, d).wait_send()
            sib_copy(d, i).wait()

    @pl.loop(0, NS)
    def _(s):
        for d in range(2):
            fw_copy(d, s).wait_send()
            fw_sib(d, s).wait()


def solution(mesh):
    tp = mesh.shape["tp"]

    def local(x, w, r, g):
        t, f = x.shape
        h = w.shape[1]
        blk = t // (2 * tp)
        dma = pltpu.SemaphoreType.DMA
        bf16 = jnp.bfloat16
        any_spec = pl.BlockSpec(memory_space=pl.ANY)
        return pl.pallas_call(
            functools.partial(kernel, tp),
            out_shape=jax.ShapeDtypeStruct((t, h), bf16),
            in_specs=[any_spec] * 4,
            out_specs=any_spec,
            scratch_shapes=[
                pltpu.VMEM((2, 4, blk, f), bf16),
                pltpu.VMEM((NC, f, h // NC), bf16),
                pltpu.VMEM((1, h), bf16),
                pltpu.VMEM((2 * blk, h), bf16),
                pltpu.VMEM((4, blk, h // NC), bf16),
                pltpu.VMEM((8, blk, h), bf16),
                pltpu.VMEM((6, blk, h), bf16),
                dma((2, 4)), dma((NC,)), dma((2,)),
                dma((4,)), dma((8 * NC,)),
                dma((4 * NC,)), dma((4 * NC,)),
                dma((2 * NS,)), dma((2 * NS,)),
                dma((2, 2 * NS)), dma((2, 2 * NS)),
                dma((2, NS)), dma((2, NS)),
                dma((4, 2 * NS)), dma((4, 2 * NS)),
                dma((2 * NS,)),
            ],
            compiler_params=pltpu.CompilerParams(
                collective_id=0, has_side_effects=True, vmem_limit_bytes=67043328,
            ),
            cost_estimate=pl.CostEstimate(
                flops=2 * t * f * h, bytes_accessed=2 * (t * f + f * h + 3 * t * h), transcendentals=0
            ),
        )(x, w, r, g.reshape(1, h))

    return jax.shard_map(
        local,
        mesh=mesh,
        in_specs=(P("data", "tp"), P("tp", None), P("data", None), P(None)),
        out_specs=P("data", None),
        check_vma=False,
    )
```

```python
import functools

import jax
import jax.numpy as jnp
from jax import lax
from jax.experimental import pallas as pl
from jax.experimental.pallas import tpu as pltpu
from jax.sharding import PartitionSpec as P

EPS = 1e-6
MESH = pl.DeviceIdType.MESH
NC = 4
NS = 4
VMEM_COMM = 30 * 1024 * 1024
VMEM_WRITE = 1024 * 1024


def kernel(
    tp, x, w, r, g, out,
    xbuf, wbuf, gbuf, rbuf, stage,
    x_sem, w_sem, g_sem, pair_s, pair_r, rs_s, rs_r, cb_s, cb_r,
    ag_s, ag_r, fw_s, fw_r, sib_s, sib_r, ready,
):
    n = tp // 2
    blk = stage.shape[1]
    cols = wbuf.shape[2]
    sub = blk // NS
    me = lax.axis_index("tp")
    chip = me // 2
    core = me - 2 * chip
    sib = 2 * chip + 1 - core

    def chip_at(d):
        return lax.rem(chip + d + n, n)

    right = 2 * chip_at(1) + core
    left = 2 * chip_at(-1) + core

    def row_of(q, k, o):
        return pl.multiple_of(blk * (4 * q + 2 * k + o), blk)

    def remote(src, dst, ss, rs, dev):
        return pltpu.make_async_remote_copy(
            src_ref=src, dst_ref=dst, send_sem=ss, recv_sem=rs,
            device_id={"tp": dev}, device_id_type=MESH,
        )

    def part_row(job, q, k):
        pair = job // 2
        dq = jnp.where(pair == 0, -1, jnp.where(pair == 3, 0, 1))
        kk = jnp.where(pair == 2, 1 - k, k)
        return row_of(lax.rem(q + dq + n, n), kk, job - 2 * pair)

    def recv_row(job, q, k):
        pair = job // 2
        dq = jnp.where(pair == 0, 0, jnp.where(pair == 1, 2, -1))
        kk = jnp.where(pair == 1, k, 1 - k)
        return row_of(lax.rem(q + dq + n, n), kk, job - 2 * pair)

    def part(job, s, size):
        return pl.ds(pl.multiple_of(part_row(job, chip, core) + s, size), size)

    def recv(job, s, size):
        return pl.ds(pl.multiple_of(recv_row(job, chip, core) + s, size), size)

    def load_x(pair):
        res = []
        for side in range(2):
            sign = 1 - 2 * side
            q = chip_at(sign * ((4 - pair) // 2))
            o = lax.rem(side + 1 + pair, 2)
            for which in range(2):
                k = core if which == 0 else 1 - core
                slot = lax.rem(pair, 2)
                res.append(pltpu.make_async_copy(
                    x.at[pl.ds(row_of(q, k, o), blk), :],
                    xbuf.at[slot, 2 * side + which],
                    x_sem.at[slot, 2 * side + which],
                ))
        return res

    def load_w(c):
        return pltpu.make_async_copy(
            w.at[:, pl.ds(pl.multiple_of(c * cols, cols), cols)], wbuf.at[c], w_sem.at[c]
        )

    def col(c):
        return pl.ds(pl.multiple_of(c * cols, cols), cols)

    for cp in load_x(0):
        cp.start()
    for c in range(NC):
        load_w(c).start()
    for cp in load_x(1):
        cp.start()
    own0 = row_of(chip, core, 0)
    load_r = pltpu.make_async_copy(r.at[pl.ds(own0, 2 * blk), :], rbuf, g_sem.at[0])
    load_g = pltpu.make_async_copy(g, gbuf, g_sem.at[1])
    load_r.start()
    load_g.start()

    barrier = pltpu.get_barrier_semaphore()
    for dev in (sib, left, right):
        pl.semaphore_signal(barrier, inc=1, device_id={"tp": dev}, device_id_type=MESH)
    pl.semaphore_wait(barrier, 3)

    per = 2 * NC
    steps = 4 * per

    def split(t):
        pair = t // per
        c = (t - pair * per) // 2
        side = t - 2 * (t // 2)
        return pair, c, side

    def pair_copy(t):
        pair, c, side = split(t)
        return remote(
            stage.at[lax.rem(t, 4)],
            out.at[pl.ds(part_row(2 * pair + side, chip, 1 - core), blk), col(c)],
            pair_s.at[lax.rem(t, 4)], pair_r.at[t], sib,
        )

    def rs_copy(t):
        pair, c, side = split(t)
        job = 2 * pair + side
        to = chip_at(1 - 2 * side)
        return remote(
            out.at[part(job, 0, blk), col(c)],
            out.at[pl.ds(recv_row(job, to, core), blk), col(c)],
            rs_s.at[t], rs_r.at[t], 2 * to + core,
        )

    def product(pair, side, which, c):
        return jnp.dot(
            xbuf[lax.rem(pair, 2), 2 * side + which], wbuf[c],
            preferred_element_type=jnp.float32,
        )

    @pl.loop(0, steps + 1)
    def _(t):
        @pl.when(t < steps)
        def _():
            pair, c, side = split(t)

            @pl.when(lax.rem(t, per) == 0)
            def _():
                for cp in load_x(pair):
                    cp.wait()

            @pl.when(jnp.logical_and(t < per, side == 0))
            def _():
                load_w(c).wait()

            @pl.when(t >= 4)
            def _():
                pair_copy(t - 4).wait_send()

            stage[lax.rem(t, 4)] = product(pair, side, 1, c).astype(jnp.bfloat16)
            pair_copy(t).start()

        @pl.when(t > 0)
        def _():
            u = t - 1
            pair, c, side = split(u)
            job = 2 * pair + side
            pair_copy(u).wait_recv()
            acc = product(pair, side, 0, c)
            acc = acc + out[part(job, 0, blk), col(c)].astype(jnp.float32)
            out[part(job, 0, blk), col(c)] = acc.astype(jnp.bfloat16)

            @pl.when(u < 2 * per)
            def _():
                rs_copy(u).start()

            @pl.when(jnp.logical_and(lax.rem(u, per) == per - 1, pair < 2))
            def _():
                for cp in load_x(pair + 2):
                    cp.start()

    def cb_copy(i):
        s = i // 2
        side = i - 2 * s
        to = chip_at(1 - 2 * side)
        dst = pl.multiple_of(recv_row(4 + side, to, core) + s * sub, sub)
        return remote(
            out.at[part(4 + side, s * sub, sub), :], out.at[pl.ds(dst, sub), :],
            cb_s.at[i], cb_r.at[i], 2 * to + core,
        )

    @pl.loop(0, per)
    def _(t):
        rs_copy(t).wait_recv()

    @pl.loop(0, 2 * NS)
    def _(i):
        s = i // 2
        side = i - 2 * s
        total = out[part(4 + side, s * sub, sub), :].astype(jnp.float32)
        total = total + out[recv(side, s * sub, sub), :].astype(jnp.float32)
        out[part(4 + side, s * sub, sub), :] = total.astype(jnp.bfloat16)
        cb_copy(i).start()

    def tell_ready(which):
        for dev in (sib, left, right):
            pl.semaphore_signal(
                ready.at[which], inc=1, device_id={"tp": dev}, device_id_type=MESH
            )

    @pl.loop(0, 2 * per)
    def _(t):
        rs_copy(t).wait_send()

    tell_ready(0)

    @pl.loop(per, 2 * per)
    def _(t):
        rs_copy(t).wait_recv()

    load_r.wait()
    load_g.wait()
    pl.semaphore_wait(ready.at[0], 3)

    def out_rows(q, o, s, k=None):
        k = core if k is None else k
        return out.at[pl.ds(pl.multiple_of(row_of(q, k, o) + s * sub, sub), sub), :]

    def ag_copy(i, d):
        s = i // 2
        o = i - 2 * s
        return remote(
            out_rows(chip, o, s), out_rows(chip, o, s),
            ag_s.at[d, i], ag_r.at[d, i], right if d == 0 else left,
        )

    def own_sib(i):
        s = i // 2
        o = i - 2 * s
        return remote(
            out_rows(chip, o, s), out_rows(chip, o, s),
            sib_s.at[0, i], sib_r.at[0, i], sib,
        )

    grp = 16 if sub % 16 == 0 else sub

    @pl.loop(0, 2 * NS)
    def _(i):
        s = i // 2
        o = i - 2 * s
        cb_copy(2 * s + 1 - o).wait_recv()

        @pl.loop(0, sub // grp)
        def _(b):
            at = s * sub + b * grp
            y = out[part(6 + o, at, grp), :].astype(jnp.float32)
            y = y + out[recv(2 + o, at, grp), :].astype(jnp.float32)
            y = y + out[recv(5 - o, at, grp), :].astype(jnp.float32)
            rr = rbuf[pl.ds(pl.multiple_of(o * blk + at, grp), grp), :]
            a = rr.astype(jnp.float32) + y.astype(jnp.bfloat16).astype(jnp.float32)
            ms = jnp.mean(a * a, axis=-1, keepdims=True)
            z = a * lax.rsqrt(ms + EPS) * gbuf[...].astype(jnp.float32).reshape(1, -1)
            out[part(6 + o, at, grp), :] = z.astype(jnp.bfloat16)

        ag_copy(i, 0).start()
        ag_copy(i, 1).start()
        own_sib(i).start()

    @pl.loop(0, 2 * NS)
    def _(i):
        cb_copy(i).wait_send()

    tell_ready(1)
    pl.semaphore_wait(ready.at[1], 3)

    def sib_copy(d, i):
        s = i // 2
        o = i - 2 * s
        rows = out_rows(chip_at(-1 if d == 0 else 1), o, s)
        return remote(rows, rows, sib_s.at[1 + d, i], sib_r.at[1 + d, i], sib)

    def fw_copy(d, s):
        rows = out_rows(chip_at(-1 if d == 0 else 1), d, s)
        return remote(rows, rows, fw_s.at[d, s], fw_r.at[d, s], right if d == 0 else left)

    def fw_sib(d, s):
        rows = out_rows(chip_at(2), d, s)
        return remote(rows, rows, sib_s.at[3, 2 * s + d], sib_r.at[3, 2 * s + d], sib)

    @pl.loop(0, NS)
    def _(s):
        for o in range(2):
            i = 2 * s + o
            for d in range(2):
                ag_copy(i, d).wait_recv()
                if o == d:
                    fw_copy(d, s).start()
                sib_copy(d, i).start()

    @pl.loop(0, NS)
    def _(s):
        for d in range(2):
            rows = out_rows(chip_at(2), d, s)
            remote(rows, rows, fw_s.at[d, s], fw_r.at[d, s], sib).wait_recv()
            fw_sib(d, s).start()

    @pl.loop(steps - 4, steps)
    def _(t):
        pair_copy(t).wait_send()

    @pl.loop(0, 2 * NS)
    def _(i):
        own_sib(i).wait()
        for d in range(2):
            ag_copy(i, d).wait_send()
            sib_copy(d, i).wait()

    @pl.loop(0, NS)
    def _(s):
        for d in range(2):
            fw_copy(d, s).wait_send()
            fw_sib(d, s).wait()


def write_out(z, o, sem):
    rows = z.shape[0] // sem.shape[0]
    copies = [
        pltpu.make_async_copy(z.at[pl.ds(i * rows, rows), :], o.at[pl.ds(i * rows, rows), :], sem.at[i])
        for i in range(sem.shape[0])
    ]
    for cp in copies:
        cp.start()
    for cp in copies:
        cp.wait()


def solution(mesh):
    tp = mesh.shape["tp"]

    def local(x, w, r, g):
        t, f = x.shape
        h = w.shape[1]
        blk = t // (2 * tp)
        dma = pltpu.SemaphoreType.DMA
        bf16 = jnp.bfloat16
        any_spec = pl.BlockSpec(memory_space=pl.ANY)
        z = pl.pallas_call(
            functools.partial(kernel, tp),
            out_shape=pltpu.VMEM((t, h), bf16),
            in_specs=[any_spec] * 4,
            out_specs=pl.BlockSpec(memory_space=pltpu.VMEM),
            scratch_shapes=[
                pltpu.VMEM((2, 4, blk, f), bf16),
                pltpu.VMEM((NC, f, h // NC), bf16),
                pltpu.VMEM((h,), bf16),
                pltpu.VMEM((2 * blk, h), bf16),
                pltpu.VMEM((4, blk, h // NC), bf16),
                dma((2, 4)), dma((NC,)), dma((2,)),
                dma((4,)), dma((8 * NC,)),
                dma((4 * NC,)), dma((4 * NC,)),
                dma((2 * NS,)), dma((2 * NS,)),
                dma((2, 2 * NS)), dma((2, 2 * NS)),
                dma((2, NS)), dma((2, NS)),
                dma((4, 2 * NS)), dma((4, 2 * NS)),
                pltpu.SemaphoreType.REGULAR((2,)),
            ],
            compiler_params=pltpu.CompilerParams(
                collective_id=0, has_side_effects=True, vmem_limit_bytes=VMEM_COMM,
            ),
            cost_estimate=pl.CostEstimate(
                flops=2 * t * f * h, bytes_accessed=2 * (t * f + f * h + 2 * t * h), transcendentals=0
            ),
        )(x, w, r, g)
        return pl.pallas_call(
            write_out,
            out_shape=jax.ShapeDtypeStruct((t, h), bf16),
            in_specs=[pl.BlockSpec(memory_space=pltpu.VMEM)],
            out_specs=any_spec,
            scratch_shapes=[dma((16,))],
            compiler_params=pltpu.CompilerParams(vmem_limit_bytes=VMEM_WRITE),
        )(z)

    return jax.shard_map(
        local,
        mesh=mesh,
        in_specs=(P("data", "tp"), P("tp", None), P("data", None), P(None)),
        out_specs=P("data", None),
        check_vma=False,
    )
```

```python
import functools

import jax
import jax.numpy as jnp
from jax import lax
from jax.experimental import pallas as pl
from jax.experimental.pallas import tpu as pltpu
from jax.sharding import PartitionSpec as P

EPS = 1e-6
MESH = pl.DeviceIdType.MESH
NC = 8
NS = 4
VMEM_COMM = 30 * 1024 * 1024
VMEM_WRITE = 1024 * 1024


def kernel(
    tp, x, w, r, g, out,
    xbuf, wbuf, gbuf, rbuf, stage,
    x_sem, w_sem, g_sem, pair_s, pair_r, rs_s, rs_r, cb_s, cb_r,
    ag_s, ag_r, fw_s, fw_r, ts_s, ts_r, sib_s, sib_r, ready,
):
    n = tp // 2
    blk = stage.shape[1] // 2
    cols = wbuf.shape[2]
    sub = blk // NS
    me = lax.axis_index("tp")
    chip = me // 2
    core = me - 2 * chip
    sib = 2 * chip + 1 - core

    def chip_at(d):
        return lax.rem(chip + d + n, n)

    right = 2 * chip_at(1) + core
    left = 2 * chip_at(-1) + core

    def row_of(q, k, o):
        return pl.multiple_of(blk * (4 * q + 2 * k + o), blk)

    def remote(src, dst, ss, rs, dev):
        return pltpu.make_async_remote_copy(
            src_ref=src, dst_ref=dst, send_sem=ss, recv_sem=rs,
            device_id={"tp": dev}, device_id_type=MESH,
        )

    def part_row(job, q, k):
        pair = job // 2
        dq = jnp.where(pair == 0, -1, jnp.where(pair == 3, 0, 1))
        kk = jnp.where(pair == 2, 1 - k, k)
        return row_of(lax.rem(q + dq + n, n), kk, job - 2 * pair)

    def recv_row(job, q, k):
        pair = job // 2
        dq = jnp.where(pair == 0, 0, jnp.where(pair == 1, 2, -1))
        kk = jnp.where(pair == 1, k, 1 - k)
        return row_of(lax.rem(q + dq + n, n), kk, job - 2 * pair)

    def part(job, s, size):
        return pl.ds(pl.multiple_of(part_row(job, chip, core) + s, size), size)

    def recv(job, s, size):
        return pl.ds(pl.multiple_of(recv_row(job, chip, core) + s, size), size)

    def load_x(pair, side, which):
        q = chip_at((1 - 2 * side) * ((4 - pair) // 2))
        o = lax.rem(side + 1 + pair, 2)
        k = core if which == 0 else 1 - core
        slot = lax.rem(pair, 2)
        return pltpu.make_async_copy(
            x.at[pl.ds(row_of(q, k, o), blk), :],
            xbuf.at[slot, which, pl.ds(side * blk, blk), :],
            x_sem.at[slot, which, side],
        )

    def load_w(c):
        return pltpu.make_async_copy(
            w.at[:, pl.ds(pl.multiple_of(c * cols, cols), cols)], wbuf.at[c], w_sem.at[c]
        )

    def col(c):
        return pl.ds(pl.multiple_of(c * cols, cols), cols)

    def start_x(pair, which):
        for side in range(2):
            load_x(pair, side, which).start()

    def wait_x(pair, which):
        for side in range(2):
            load_x(pair, side, which).wait()

    pieces = ((0, cols // 4), (cols // 4, cols - cols // 4))

    def load_w0(i):
        at, size = pieces[i]
        return pltpu.make_async_copy(
            w.at[:, pl.ds(at, size)], wbuf.at[0, :, pl.ds(at, size)], w_sem.at[i * NC]
        )

    start_x(0, 1)
    load_w0(0).start()
    start_x(0, 0)
    load_w0(1).start()
    load_w(1).start()
    own0 = row_of(chip, core, 0)
    load_r = pltpu.make_async_copy(r.at[pl.ds(own0, 2 * blk), :], rbuf, g_sem.at[0])
    load_g = pltpu.make_async_copy(g, gbuf, g_sem.at[1])

    barrier = pltpu.get_barrier_semaphore()
    for dev in (sib, left, right):
        pl.semaphore_signal(barrier, inc=1, device_id={"tp": dev}, device_id_type=MESH)

    steps = 4 * NC

    def pair_copy(t, side):
        pair = t // NC
        slot = lax.rem(t, 4)
        return remote(
            stage.at[slot, pl.ds(side * blk, blk), :],
            out.at[pl.ds(part_row(2 * pair + side, chip, 1 - core), blk), col(t - pair * NC)],
            pair_s.at[slot, side], pair_r.at[t, side], sib,
        )

    def far_copy(c, side):
        to = chip_at(1 - 2 * side)
        return remote(
            out.at[part(side, 0, blk), col(c)],
            out.at[pl.ds(recv_row(side, to, core), blk), col(c)],
            rs_s.at[side, c], rs_r.at[side, c], 2 * to + core,
        )

    def near_copy(side):
        to = chip_at(1 - 2 * side)
        return remote(
            out.at[part(2 + side, 0, blk), :],
            out.at[pl.ds(recv_row(2 + side, to, core), blk), :],
            rs_s.at[side, NC], rs_r.at[side, NC], 2 * to + core,
        )

    def product(pair, which, c):
        return jnp.dot(
            xbuf[lax.rem(pair, 2), which], wbuf[c], preferred_element_type=jnp.float32
        )

    def give(t):
        pair = t // NC
        stage[lax.rem(t, 4)] = product(pair, 1, t - pair * NC).astype(jnp.bfloat16)

    def start_give(t):
        for side in range(2):
            pair_copy(t, side).start()

    def take(t):
        pair = t // NC
        c = t - pair * NC
        acc = product(pair, 0, c)
        for side in range(2):
            pair_copy(t, side).wait_recv()
            rows = part(2 * pair + side, 0, blk)
            both = acc[side * blk:(side + 1) * blk] + out[rows, col(c)].astype(jnp.float32)
            out[rows, col(c)] = both.astype(jnp.bfloat16)

            @pl.when(pair == 0)
            def _():
                far_copy(c, side).start()

            @pl.when(jnp.logical_and(pair == 1, c == NC - 1))
            def _():
                near_copy(side).start()

    def first_pair(i, side):
        at, size = pieces[i]
        return remote(
            stage.at[0, pl.ds(side * blk, blk), pl.ds(at, size)],
            out.at[pl.ds(part_row(side, chip, 1 - core), blk), pl.ds(at, size)],
            pair_s.at[4 * i, side], pair_r.at[i * steps, side], sib,
        )

    def first_far(i, side):
        at, size = pieces[i]
        to = chip_at(1 - 2 * side)
        return remote(
            out.at[part(side, 0, blk), pl.ds(at, size)],
            out.at[pl.ds(recv_row(side, to, core), blk), pl.ds(at, size)],
            rs_s.at[side, i * (NC + 1)], rs_r.at[side, i * (NC + 1)], 2 * to + core,
        )

    def first_product(i, which):
        at, size = pieces[i]
        return jnp.dot(
            xbuf[0, which], wbuf[0, :, at:at + size], preferred_element_type=jnp.float32
        )

    def first_give(i):
        at, size = pieces[i]
        stage[0, :, at:at + size] = first_product(i, 1).astype(jnp.bfloat16)

    def first_take(i, acc):
        at, size = pieces[i]
        for side in range(2):
            first_pair(i, side).wait_recv()
            rows = part(side, 0, blk)
            there = out[rows, at:at + size].astype(jnp.float32)
            out[rows, at:at + size] = (acc[side * blk:(side + 1) * blk] + there).astype(jnp.bfloat16)
            first_far(i, side).start()

    wait_x(0, 1)
    load_w0(0).wait()
    first_give(0)
    pl.semaphore_wait(barrier, 3)
    for side in range(2):
        first_pair(0, side).start()
    wait_x(0, 0)
    acc = first_product(0, 0)
    load_w0(1).wait()
    load_w(2).start()
    first_give(1)
    for side in range(2):
        first_pair(1, side).start()
    first_take(0, acc)
    first_take(1, first_product(1, 0))
    for i in range(2):
        for side in range(2):
            first_pair(i, side).wait_send()

    @pl.loop(1, steps + 1)
    def _(t):
        @pl.when(t < steps)
        def _():
            pair = t // NC
            c = t - pair * NC

            @pl.when(c == 0)
            def _():
                wait_x(pair, 1)

            @pl.when(t < NC)
            def _():
                load_w(c).wait()

            @pl.when(t < NC - 2)
            def _():
                load_w(c + 2).start()

            @pl.when(t == NC // 2)
            def _():
                start_x(1, 1)
                start_x(1, 0)
                load_r.start()
                load_g.start()

            @pl.when(t > 4)
            def _():
                for side in range(2):
                    pair_copy(t - 4, side).wait_send()

            give(t)
            start_give(t)

        @pl.when(t > 1)
        def _():
            u = t - 1
            pair = u // NC
            c = u - pair * NC

            @pl.when(c == 0)
            def _():
                wait_x(pair, 0)

            take(u)

            @pl.when(jnp.logical_and(c == NC - 1, pair < 2))
            def _():
                start_x(pair + 2, 1)
                start_x(pair + 2, 0)

    def cb_copy(i):
        s = i // 2
        side = i - 2 * s
        to = chip_at(1 - 2 * side)
        dst = pl.multiple_of(recv_row(4 + side, to, core) + s * sub, sub)
        return remote(
            out.at[part(4 + side, s * sub, sub), :], out.at[pl.ds(dst, sub), :],
            cb_s.at[i], cb_r.at[i], 2 * to + core,
        )

    for i in range(2):
        for side in range(2):
            first_far(i, side).wait_recv()

    @pl.loop(1, NC)
    def _(c):
        for side in range(2):
            far_copy(c, side).wait_recv()

    @pl.loop(0, 2 * NS)
    def _(i):
        s = i // 2
        side = i - 2 * s
        total = out[part(4 + side, s * sub, sub), :].astype(jnp.float32)
        total = total + out[recv(side, s * sub, sub), :].astype(jnp.float32)
        out[part(4 + side, s * sub, sub), :] = total.astype(jnp.bfloat16)
        cb_copy(i).start()

    def tell_ready(which):
        for dev in (sib, left, right):
            pl.semaphore_signal(
                ready.at[which], inc=1, device_id={"tp": dev}, device_id_type=MESH
            )

    for i in range(2):
        for side in range(2):
            first_far(i, side).wait_send()

    @pl.loop(1, NC)
    def _(c):
        for side in range(2):
            far_copy(c, side).wait_send()

    for side in range(2):
        near_copy(side).wait_send()

    @pl.loop(steps - 4, steps)
    def _(t):
        for side in range(2):
            pair_copy(t, side).wait_send()

    tell_ready(0)

    for side in range(2):
        near_copy(side).wait_recv()

    load_r.wait()
    load_g.wait()
    pl.semaphore_wait(ready.at[0], 3)

    def out_rows(q, o, s, k=None):
        k = core if k is None else k
        return out.at[pl.ds(pl.multiple_of(row_of(q, k, o) + s * sub, sub), sub), :]

    def ag_copy(i, d):
        s = i // 2
        o = i - 2 * s
        return remote(
            out_rows(chip, o, s), out_rows(chip, o, s),
            ag_s.at[d, i], ag_r.at[d, i], right if d == 0 else left,
        )

    def own_sib(i):
        s = i // 2
        o = i - 2 * s
        return remote(
            out_rows(chip, o, s), out_rows(chip, o, s),
            sib_s.at[0, i], sib_r.at[0, i], sib,
        )

    grp = 16 if sub % 16 == 0 else sub

    @pl.loop(0, 2 * NS)
    def _(i):
        s = i // 2
        o = i - 2 * s
        cb_copy(2 * s + 1 - o).wait_recv()

        @pl.loop(0, sub // grp)
        def _(b):
            at = s * sub + b * grp
            y = out[part(6 + o, at, grp), :].astype(jnp.float32)
            y = y + out[recv(2 + o, at, grp), :].astype(jnp.float32)
            y = y + out[recv(5 - o, at, grp), :].astype(jnp.float32)
            rr = rbuf[pl.ds(pl.multiple_of(o * blk + at, grp), grp), :]
            a = rr.astype(jnp.float32) + y.astype(jnp.bfloat16).astype(jnp.float32)
            ms = jnp.mean(a * a, axis=-1, keepdims=True)
            z = a * lax.rsqrt(ms + EPS) * gbuf[...].astype(jnp.float32).reshape(1, -1)
            out[part(6 + o, at, grp), :] = z.astype(jnp.bfloat16)

        ag_copy(i, 0).start()
        ag_copy(i, 1).start()
        own_sib(i).start()

    @pl.loop(0, 2 * NS)
    def _(i):
        cb_copy(i).wait_send()

    tell_ready(1)
    pl.semaphore_wait(ready.at[1], 3)

    def sib_copy(d, i):
        s = i // 2
        o = i - 2 * s
        rows = out_rows(chip_at(-1 if d == 0 else 1), o, s)
        return remote(rows, rows, sib_s.at[1 + d, i], sib_r.at[1 + d, i], sib)

    tail = [(s * sub, sub) for s in range(NS - 1)]
    tail += [(blk - sub, sub // 2), (blk - sub // 2, sub // 4), (blk - sub // 4, sub // 4)]

    def fw_rows(q, d, p):
        at, size = tail[p]
        return out.at[pl.ds(pl.multiple_of(row_of(q, core, d) + at, size), size), :]

    def fw_copy(d, p):
        rows = fw_rows(chip_at(-1 if d == 0 else 1), d, p)
        return remote(rows, rows, fw_s.at[d, p], fw_r.at[d, p], right if d == 0 else left)

    def fw_in(d, p):
        rows = fw_rows(chip_at(2), d, p)
        return remote(rows, rows, fw_s.at[d, p], fw_r.at[d, p], sib)

    def fw_sib(d, p):
        rows = fw_rows(chip_at(2), d, p)
        return remote(rows, rows, ts_s.at[d, p], ts_r.at[d, p], sib)

    for s in range(NS):
        for o in range(2):
            i = 2 * s + o
            for d in range(2):
                ag_copy(i, d).wait_recv()
                if o == d:
                    for p in range(s, len(tail) if s == NS - 1 else s + 1):
                        fw_copy(d, p).start()
                sib_copy(d, i).start()

    @pl.loop(0, 2 * NS)
    def _(i):
        own_sib(i).wait()
        for d in range(2):
            ag_copy(i, d).wait_send()
            sib_copy(d, i).wait()

    for p in range(len(tail)):
        for d in range(2):
            fw_in(d, p).wait_recv()
            fw_sib(d, p).start()
            fw_copy(d, p).wait_send()
            if p:
                fw_sib(d, p - 1).wait()

    for d in range(2):
        fw_sib(d, len(tail) - 1).wait()


def write_out(z, o, sem):
    rows = z.shape[0] // sem.shape[0]
    copies = [
        pltpu.make_async_copy(z.at[pl.ds(i * rows, rows), :], o.at[pl.ds(i * rows, rows), :], sem.at[i])
        for i in range(sem.shape[0])
    ]
    for cp in copies:
        cp.start()
    for cp in copies:
        cp.wait()


def solution(mesh):
    tp = mesh.shape["tp"]

    def local(x, w, r, g):
        t, f = x.shape
        h = w.shape[1]
        blk = t // (2 * tp)
        dma = pltpu.SemaphoreType.DMA
        bf16 = jnp.bfloat16
        any_spec = pl.BlockSpec(memory_space=pl.ANY)
        z = pl.pallas_call(
            functools.partial(kernel, tp),
            out_shape=pltpu.VMEM((t, h), bf16),
            in_specs=[any_spec] * 4,
            out_specs=pl.BlockSpec(memory_space=pltpu.VMEM),
            scratch_shapes=[
                pltpu.VMEM((2, 2, 2 * blk, f), bf16),
                pltpu.VMEM((NC, f, h // NC), bf16),
                pltpu.VMEM((h,), bf16),
                pltpu.VMEM((2 * blk, h), bf16),
                pltpu.VMEM((4, 2 * blk, h // NC), bf16),
                dma((2, 2, 2)), dma((NC + 1,)), dma((2,)),
                dma((5, 2)), dma((4 * NC + 1, 2)),
                dma((2, NC + 2)), dma((2, NC + 2)),
                dma((2 * NS,)), dma((2 * NS,)),
                dma((2, 2 * NS)), dma((2, 2 * NS)),
                dma((2, NS + 2)), dma((2, NS + 2)),
                dma((2, NS + 2)), dma((2, NS + 2)),
                dma((3, 2 * NS)), dma((3, 2 * NS)),
                pltpu.SemaphoreType.REGULAR((2,)),
            ],
            compiler_params=pltpu.CompilerParams(
                collective_id=0, has_side_effects=True, vmem_limit_bytes=VMEM_COMM,
            ),
            cost_estimate=pl.CostEstimate(
                flops=2 * t * f * h, bytes_accessed=2 * (t * f + f * h + 2 * t * h), transcendentals=0
            ),
        )(x, w, r, g)
        return pl.pallas_call(
            write_out,
            out_shape=jax.ShapeDtypeStruct((t, h), bf16),
            in_specs=[pl.BlockSpec(memory_space=pltpu.VMEM)],
            out_specs=any_spec,
            scratch_shapes=[dma((16,))],
            compiler_params=pltpu.CompilerParams(vmem_limit_bytes=VMEM_WRITE),
        )(z)

    return jax.shard_map(
        local,
        mesh=mesh,
        in_specs=(P("data", "tp"), P("tp", None), P("data", None), P(None)),
        out_specs=P("data", None),
        check_vma=False,
    )
```

```python
import functools

import jax
import jax.numpy as jnp
from jax import lax
from jax.experimental import pallas as pl
from jax.experimental.pallas import tpu as pltpu
from jax.sharding import PartitionSpec as P

EPS = 1e-6
MESH = pl.DeviceIdType.MESH
NC = 8
NS = 4
VMEM_COMM = 30 * 1024 * 1024
VMEM_WRITE = 1024 * 1024


def kernel(
    tp, x, w, r, g, out,
    xbuf, wbuf, gbuf, rbuf, stage,
    x_sem, w_sem, g_sem, pair_s, pair_r, rs_s, rs_r, cb_s, cb_r,
    ag_s, ag_r, fw_s, fw_r, ts_s, ts_r, sib_s, sib_r, ready,
):
    n = tp // 2
    blk = stage.shape[1] // 2
    cols = wbuf.shape[2]
    sub = blk // NS
    me = lax.axis_index("tp")
    chip = me // 2
    core = me - 2 * chip
    sib = 2 * chip + 1 - core

    def chip_at(d):
        return lax.rem(chip + d + n, n)

    right = 2 * chip_at(1) + core
    left = 2 * chip_at(-1) + core

    def row_of(q, k, o):
        return pl.multiple_of(blk * (4 * q + 2 * k + o), blk)

    def remote(src, dst, ss, rs, dev):
        return pltpu.make_async_remote_copy(
            src_ref=src, dst_ref=dst, send_sem=ss, recv_sem=rs,
            device_id={"tp": dev}, device_id_type=MESH,
        )

    def part_row(job, q, k):
        pair = job // 2
        dq = jnp.where(pair == 0, -1, jnp.where(pair == 3, 0, 1))
        kk = jnp.where(pair == 2, 1 - k, k)
        return row_of(lax.rem(q + dq + n, n), kk, job - 2 * pair)

    def recv_row(job, q, k):
        pair = job // 2
        dq = jnp.where(pair == 0, 0, jnp.where(pair == 1, 2, -1))
        kk = jnp.where(pair == 1, k, 1 - k)
        return row_of(lax.rem(q + dq + n, n), kk, job - 2 * pair)

    def part(job, s, size):
        return pl.ds(pl.multiple_of(part_row(job, chip, core) + s, size), size)

    def recv(job, s, size):
        return pl.ds(pl.multiple_of(recv_row(job, chip, core) + s, size), size)

    def load_x(pair, side, which):
        q = chip_at((1 - 2 * side) * ((4 - pair) // 2))
        o = lax.rem(side + 1 + pair, 2)
        k = core if which == 0 else 1 - core
        slot = lax.rem(pair, 2)
        return pltpu.make_async_copy(
            x.at[pl.ds(row_of(q, k, o), blk), :],
            xbuf.at[slot, which, pl.ds(side * blk, blk), :],
            x_sem.at[slot, which, side],
        )

    def load_w(c):
        return pltpu.make_async_copy(
            w.at[:, pl.ds(pl.multiple_of(c * cols, cols), cols)], wbuf.at[c], w_sem.at[c]
        )

    def col(c):
        return pl.ds(pl.multiple_of(c * cols, cols), cols)

    def start_x(pair, which):
        for side in range(2):
            load_x(pair, side, which).start()

    def wait_x(pair, which):
        for side in range(2):
            load_x(pair, side, which).wait()

    pieces = ((0, cols // 2), (cols // 2, cols - cols // 2))

    def load_w0(i):
        at, size = pieces[i]
        return pltpu.make_async_copy(
            w.at[:, pl.ds(at, size)], wbuf.at[0, :, pl.ds(at, size)], w_sem.at[i * NC]
        )

    start_x(0, 1)
    load_w0(0).start()
    start_x(0, 0)
    load_w0(1).start()
    load_w(1).start()
    own0 = row_of(chip, core, 0)
    load_r = pltpu.make_async_copy(r.at[pl.ds(own0, 2 * blk), :], rbuf, g_sem.at[0])
    load_g = pltpu.make_async_copy(g, gbuf, g_sem.at[1])

    barrier = pltpu.get_barrier_semaphore()
    for dev in (sib, left, right):
        pl.semaphore_signal(barrier, inc=1, device_id={"tp": dev}, device_id_type=MESH)

    steps = 4 * NC

    def pair_copy(t, side):
        pair = t // NC
        slot = lax.rem(t, 4)
        return remote(
            stage.at[slot, pl.ds(side * blk, blk), :],
            out.at[pl.ds(part_row(2 * pair + side, chip, 1 - core), blk), col(t - pair * NC)],
            pair_s.at[slot, side], pair_r.at[t, side], sib,
        )

    def far_copy(c, side):
        to = chip_at(1 - 2 * side)
        return remote(
            out.at[part(side, 0, blk), col(c)],
            out.at[pl.ds(recv_row(side, to, core), blk), col(c)],
            rs_s.at[side, c], rs_r.at[side, c], 2 * to + core,
        )

    def near_copy(side):
        to = chip_at(1 - 2 * side)
        return remote(
            out.at[part(2 + side, 0, blk), :],
            out.at[pl.ds(recv_row(2 + side, to, core), blk), :],
            rs_s.at[side, NC], rs_r.at[side, NC], 2 * to + core,
        )

    def product(pair, which, c):
        return jnp.dot(
            xbuf[lax.rem(pair, 2), which], wbuf[c], preferred_element_type=jnp.float32
        )

    def give(t):
        pair = t // NC
        stage[lax.rem(t, 4)] = product(pair, 1, t - pair * NC).astype(jnp.bfloat16)

    def start_give(t):
        for side in range(2):
            pair_copy(t, side).start()

    def take(t):
        pair = t // NC
        c = t - pair * NC
        acc = product(pair, 0, c)
        for side in range(2):
            pair_copy(t, side).wait_recv()
            rows = part(2 * pair + side, 0, blk)
            both = acc[side * blk:(side + 1) * blk] + out[rows, col(c)].astype(jnp.float32)
            out[rows, col(c)] = both.astype(jnp.bfloat16)

            @pl.when(pair == 0)
            def _():
                far_copy(c, side).start()

            @pl.when(jnp.logical_and(pair == 1, c == NC - 1))
            def _():
                near_copy(side).start()

    def first_pair(i, side):
        at, size = pieces[i]
        return remote(
            stage.at[0, pl.ds(side * blk, blk), pl.ds(at, size)],
            out.at[pl.ds(part_row(side, chip, 1 - core), blk), pl.ds(at, size)],
            pair_s.at[4 * i, side], pair_r.at[i * steps, side], sib,
        )

    def first_far(i, side):
        at, size = pieces[i]
        to = chip_at(1 - 2 * side)
        return remote(
            out.at[part(side, 0, blk), pl.ds(at, size)],
            out.at[pl.ds(recv_row(side, to, core), blk), pl.ds(at, size)],
            rs_s.at[side, i * (NC + 1)], rs_r.at[side, i * (NC + 1)], 2 * to + core,
        )

    def first_product(i, which):
        at, size = pieces[i]
        return jnp.dot(
            xbuf[0, which], wbuf[0, :, at:at + size], preferred_element_type=jnp.float32
        )

    def first_give(i):
        at, size = pieces[i]
        stage[0, :, at:at + size] = first_product(i, 1).astype(jnp.bfloat16)

    def first_take(i, acc):
        at, size = pieces[i]
        for side in range(2):
            first_pair(i, side).wait_recv()
            rows = part(side, 0, blk)
            there = out[rows, at:at + size].astype(jnp.float32)
            out[rows, at:at + size] = (acc[side * blk:(side + 1) * blk] + there).astype(jnp.bfloat16)
            first_far(i, side).start()

    wait_x(0, 1)
    load_w0(0).wait()
    first_give(0)
    pl.semaphore_wait(barrier, 3)
    for side in range(2):
        first_pair(0, side).start()
    wait_x(0, 0)
    first_take(0, first_product(0, 0))
    load_w0(1).wait()
    load_w(2).start()
    first_give(1)
    for side in range(2):
        first_pair(1, side).start()
    first_take(1, first_product(1, 0))
    for i in range(2):
        for side in range(2):
            first_pair(i, side).wait_send()

    @pl.loop(1, steps + 1)
    def _(t):
        @pl.when(t < steps)
        def _():
            pair = t // NC
            c = t - pair * NC

            @pl.when(c == 0)
            def _():
                wait_x(pair, 1)

            @pl.when(t < NC)
            def _():
                load_w(c).wait()

            @pl.when(t < NC - 2)
            def _():
                load_w(c + 2).start()

            @pl.when(t == NC // 2)
            def _():
                start_x(1, 1)
                start_x(1, 0)
                load_r.start()
                load_g.start()

            @pl.when(t > 4)
            def _():
                for side in range(2):
                    pair_copy(t - 4, side).wait_send()

            give(t)
            start_give(t)

        @pl.when(t > 1)
        def _():
            u = t - 1
            pair = u // NC
            c = u - pair * NC

            @pl.when(c == 0)
            def _():
                wait_x(pair, 0)

            take(u)

            @pl.when(jnp.logical_and(c == NC - 1, pair < 2))
            def _():
                start_x(pair + 2, 1)
                start_x(pair + 2, 0)

    def cb_copy(i):
        s = i // 2
        side = i - 2 * s
        to = chip_at(1 - 2 * side)
        dst = pl.multiple_of(recv_row(4 + side, to, core) + s * sub, sub)
        return remote(
            out.at[part(4 + side, s * sub, sub), :], out.at[pl.ds(dst, sub), :],
            cb_s.at[i], cb_r.at[i], 2 * to + core,
        )

    for i in range(2):
        for side in range(2):
            first_far(i, side).wait_recv()

    @pl.loop(1, NC)
    def _(c):
        for side in range(2):
            far_copy(c, side).wait_recv()

    @pl.loop(0, 2 * NS)
    def _(i):
        s = i // 2
        side = i - 2 * s
        total = out[part(4 + side, s * sub, sub), :].astype(jnp.float32)
        total = total + out[recv(side, s * sub, sub), :].astype(jnp.float32)
        out[part(4 + side, s * sub, sub), :] = total.astype(jnp.bfloat16)
        cb_copy(i).start()

    def tell_ready(which):
        for dev in (sib, left, right):
            pl.semaphore_signal(
                ready.at[which], inc=1, device_id={"tp": dev}, device_id_type=MESH
            )

    for i in range(2):
        for side in range(2):
            first_far(i, side).wait_send()

    @pl.loop(1, NC)
    def _(c):
        for side in range(2):
            far_copy(c, side).wait_send()

    for side in range(2):
        near_copy(side).wait_send()

    @pl.loop(steps - 4, steps)
    def _(t):
        for side in range(2):
            pair_copy(t, side).wait_send()

    tell_ready(0)

    for side in range(2):
        near_copy(side).wait_recv()

    load_r.wait()
    load_g.wait()
    pl.semaphore_wait(ready.at[0], 3)

    def out_rows(q, o, s, k=None):
        k = core if k is None else k
        return out.at[pl.ds(pl.multiple_of(row_of(q, k, o) + s * sub, sub), sub), :]

    def ag_copy(i, d):
        s = i // 2
        o = i - 2 * s
        return remote(
            out_rows(chip, o, s), out_rows(chip, o, s),
            ag_s.at[d, i], ag_r.at[d, i], right if d == 0 else left,
        )

    def own_sib(i):
        s = i // 2
        o = i - 2 * s
        return remote(
            out_rows(chip, o, s), out_rows(chip, o, s),
            sib_s.at[0, i], sib_r.at[0, i], sib,
        )

    grp = 16 if sub % 16 == 0 else sub

    @pl.loop(0, 2 * NS)
    def _(i):
        s = i // 2
        o = i - 2 * s
        cb_copy(2 * s + 1 - o).wait_recv()

        @pl.loop(0, sub // grp)
        def _(b):
            at = s * sub + b * grp
            y = out[part(6 + o, at, grp), :].astype(jnp.float32)
            y = y + out[recv(2 + o, at, grp), :].astype(jnp.float32)
            y = y + out[recv(5 - o, at, grp), :].astype(jnp.float32)
            rr = rbuf[pl.ds(pl.multiple_of(o * blk + at, grp), grp), :]
            a = rr.astype(jnp.float32) + y.astype(jnp.bfloat16).astype(jnp.float32)
            ms = jnp.mean(a * a, axis=-1, keepdims=True)
            z = a * lax.rsqrt(ms + EPS) * gbuf[...].astype(jnp.float32).reshape(1, -1)
            out[part(6 + o, at, grp), :] = z.astype(jnp.bfloat16)

        ag_copy(i, 0).start()
        ag_copy(i, 1).start()
        own_sib(i).start()

    @pl.loop(0, 2 * NS)
    def _(i):
        cb_copy(i).wait_send()

    tell_ready(1)
    pl.semaphore_wait(ready.at[1], 3)

    def sib_copy(d, i):
        s = i // 2
        o = i - 2 * s
        rows = out_rows(chip_at(-1 if d == 0 else 1), o, s)
        return remote(rows, rows, sib_s.at[1 + d, i], sib_r.at[1 + d, i], sib)

    tail = [(s * sub, sub) for s in range(NS - 1)]
    tail += [(blk - sub, sub // 2), (blk - sub // 2, sub // 4)]
    tail += [(blk - sub // 4, sub // 8), (blk - sub // 8, sub // 8)]

    def fw_rows(q, d, p):
        at, size = tail[p]
        return out.at[pl.ds(pl.multiple_of(row_of(q, core, d) + at, size), size), :]

    def fw_copy(d, p):
        rows = fw_rows(chip_at(-1 if d == 0 else 1), d, p)
        return remote(rows, rows, fw_s.at[d, p], fw_r.at[d, p], right if d == 0 else left)

    def fw_in(d, p):
        rows = fw_rows(chip_at(2), d, p)
        return remote(rows, rows, fw_s.at[d, p], fw_r.at[d, p], sib)

    def fw_sib(d, p):
        rows = fw_rows(chip_at(2), d, p)
        return remote(rows, rows, ts_s.at[d, p], ts_r.at[d, p], sib)

    for s in range(NS):
        for o in range(2):
            i = 2 * s + o
            for d in range(2):
                ag_copy(i, d).wait_recv()
                if o == d:
                    for p in range(s, len(tail) if s == NS - 1 else s + 1):
                        fw_copy(d, p).start()
                sib_copy(d, i).start()

    @pl.loop(0, 2 * NS)
    def _(i):
        own_sib(i).wait()
        for d in range(2):
            ag_copy(i, d).wait_send()
            sib_copy(d, i).wait()

    for p in range(len(tail)):
        for d in range(2):
            fw_in(d, p).wait_recv()
            fw_sib(d, p).start()
            fw_copy(d, p).wait_send()
            if p:
                fw_sib(d, p - 1).wait()

    for d in range(2):
        fw_sib(d, len(tail) - 1).wait()


def write_out(z, o, sem):
    rows = z.shape[0] // sem.shape[0]
    copies = [
        pltpu.make_async_copy(z.at[pl.ds(i * rows, rows), :], o.at[pl.ds(i * rows, rows), :], sem.at[i])
        for i in range(sem.shape[0])
    ]
    for cp in copies:
        cp.start()
    for cp in copies:
        cp.wait()


def solution(mesh):
    tp = mesh.shape["tp"]

    def local(x, w, r, g):
        t, f = x.shape
        h = w.shape[1]
        blk = t // (2 * tp)
        dma = pltpu.SemaphoreType.DMA
        bf16 = jnp.bfloat16
        any_spec = pl.BlockSpec(memory_space=pl.ANY)
        z = pl.pallas_call(
            functools.partial(kernel, tp),
            out_shape=pltpu.VMEM((t, h), bf16),
            in_specs=[any_spec] * 4,
            out_specs=pl.BlockSpec(memory_space=pltpu.VMEM),
            scratch_shapes=[
                pltpu.VMEM((2, 2, 2 * blk, f), bf16),
                pltpu.VMEM((NC, f, h // NC), bf16),
                pltpu.VMEM((h,), bf16),
                pltpu.VMEM((2 * blk, h), bf16),
                pltpu.VMEM((4, 2 * blk, h // NC), bf16),
                dma((2, 2, 2)), dma((NC + 1,)), dma((2,)),
                dma((5, 2)), dma((4 * NC + 1, 2)),
                dma((2, NC + 2)), dma((2, NC + 2)),
                dma((2 * NS,)), dma((2 * NS,)),
                dma((2, 2 * NS)), dma((2, 2 * NS)),
                dma((2, NS + 3)), dma((2, NS + 3)),
                dma((2, NS + 3)), dma((2, NS + 3)),
                dma((3, 2 * NS)), dma((3, 2 * NS)),
                pltpu.SemaphoreType.REGULAR((2,)),
            ],
            compiler_params=pltpu.CompilerParams(
                collective_id=0, has_side_effects=True, vmem_limit_bytes=VMEM_COMM,
            ),
            cost_estimate=pl.CostEstimate(
                flops=2 * t * f * h, bytes_accessed=2 * (t * f + f * h + 2 * t * h), transcendentals=0
            ),
        )(x, w, r, g)
        return pl.pallas_call(
            write_out,
            out_shape=jax.ShapeDtypeStruct((t, h), bf16),
            in_specs=[pl.BlockSpec(memory_space=pltpu.VMEM)],
            out_specs=any_spec,
            scratch_shapes=[dma((16,))],
            compiler_params=pltpu.CompilerParams(vmem_limit_bytes=VMEM_WRITE),
        )(z)

    return jax.shard_map(
        local,
        mesh=mesh,
        in_specs=(P("data", "tp"), P("tp", None), P("data", None), P(None)),
        out_specs=P("data", None),
        check_vma=False,
    )
```

```python
import functools

import jax
import jax.numpy as jnp
from jax import lax
from jax.experimental import pallas as pl
from jax.experimental.pallas import tpu as pltpu
from jax.sharding import PartitionSpec as P

EPS = 1e-6
MESH = pl.DeviceIdType.MESH
NC = 8
NS = 4
VMEM_COMM = 30 * 1024 * 1024
VMEM_WRITE = 1024 * 1024


def kernel(
    tp, x, w, r, g, out,
    xbuf, wbuf, gbuf, rbuf, stage,
    x_sem, w_sem, g_sem, pair_s, pair_r, rs_s, rs_r, cb_s, cb_r,
    ag_s, ag_r, fw_s, fw_r, ts_s, ts_r, sib_s, sib_r, ready,
):
    n = tp // 2
    blk = stage.shape[1] // 2
    cols = wbuf.shape[2]
    sub = blk // NS
    me = lax.axis_index("tp")
    chip = me // 2
    core = me - 2 * chip
    sib = 2 * chip + 1 - core

    def chip_at(d):
        return lax.rem(chip + d + n, n)

    right = 2 * chip_at(1) + core
    left = 2 * chip_at(-1) + core

    def row_of(q, k, o):
        return pl.multiple_of(blk * (4 * q + 2 * k + o), blk)

    def remote(src, dst, ss, rs, dev):
        return pltpu.make_async_remote_copy(
            src_ref=src, dst_ref=dst, send_sem=ss, recv_sem=rs,
            device_id={"tp": dev}, device_id_type=MESH,
        )

    def part_row(job, q, k):
        pair = job // 2
        dq = jnp.where(pair == 0, -1, jnp.where(pair == 3, 0, 1))
        kk = jnp.where(pair == 2, 1 - k, k)
        return row_of(lax.rem(q + dq + n, n), kk, job - 2 * pair)

    def recv_row(job, q, k):
        pair = job // 2
        dq = jnp.where(pair == 0, 0, jnp.where(pair == 1, 2, -1))
        kk = jnp.where(pair == 1, k, 1 - k)
        return row_of(lax.rem(q + dq + n, n), kk, job - 2 * pair)

    def part(job, s, size):
        return pl.ds(pl.multiple_of(part_row(job, chip, core) + s, size), size)

    def recv(job, s, size):
        return pl.ds(pl.multiple_of(recv_row(job, chip, core) + s, size), size)

    def load_x(pair, side, which):
        q = chip_at((1 - 2 * side) * ((4 - pair) // 2))
        o = lax.rem(side + 1 + pair, 2)
        k = core if which == 0 else 1 - core
        slot = lax.rem(pair, 2)
        return pltpu.make_async_copy(
            x.at[pl.ds(row_of(q, k, o), blk), :],
            xbuf.at[slot, which, pl.ds(side * blk, blk), :],
            x_sem.at[slot, which, side],
        )

    def load_w(c):
        return pltpu.make_async_copy(
            w.at[:, pl.ds(pl.multiple_of(c * cols, cols), cols)], wbuf.at[c], w_sem.at[c]
        )

    def col(c):
        return pl.ds(pl.multiple_of(c * cols, cols), cols)

    def start_x(pair, which):
        for side in range(2):
            load_x(pair, side, which).start()

    def wait_x(pair, which):
        for side in range(2):
            load_x(pair, side, which).wait()

    pieces = ((0, cols // 2), (cols // 2, cols - cols // 2))

    def load_w0(i):
        at, size = pieces[i]
        return pltpu.make_async_copy(
            w.at[:, pl.ds(at, size)], wbuf.at[0, :, pl.ds(at, size)], w_sem.at[i * NC]
        )

    start_x(0, 1)
    load_w0(0).start()
    start_x(0, 0)
    load_w0(1).start()
    load_w(1).start()
    own0 = row_of(chip, core, 0)
    load_r = pltpu.make_async_copy(r.at[pl.ds(own0, 2 * blk), :], rbuf, g_sem.at[0])
    load_g = pltpu.make_async_copy(g, gbuf, g_sem.at[1])

    barrier = pltpu.get_barrier_semaphore()
    for dev in (sib, left, right):
        pl.semaphore_signal(barrier, inc=1, device_id={"tp": dev}, device_id_type=MESH)

    steps = 4 * NC

    def pair_copy(t, side):
        pair = t // NC
        slot = lax.rem(t, 4)
        return remote(
            stage.at[slot, pl.ds(side * blk, blk), :],
            out.at[pl.ds(part_row(2 * pair + side, chip, 1 - core), blk), col(t - pair * NC)],
            pair_s.at[slot, side], pair_r.at[t, side], sib,
        )

    def far_copy(c, side):
        to = chip_at(1 - 2 * side)
        return remote(
            out.at[part(side, 0, blk), col(c)],
            out.at[pl.ds(recv_row(side, to, core), blk), col(c)],
            rs_s.at[side, c], rs_r.at[side, c], 2 * to + core,
        )

    def near_copy(side):
        to = chip_at(1 - 2 * side)
        return remote(
            out.at[part(2 + side, 0, blk), :],
            out.at[pl.ds(recv_row(2 + side, to, core), blk), :],
            rs_s.at[side, NC], rs_r.at[side, NC], 2 * to + core,
        )

    def product(pair, which, c):
        return jnp.dot(
            xbuf[lax.rem(pair, 2), which], wbuf[c], preferred_element_type=jnp.float32
        )

    def give(t):
        pair = t // NC
        stage[lax.rem(t, 4)] = product(pair, 1, t - pair * NC).astype(jnp.bfloat16)

    def start_give(t):
        for side in range(2):
            pair_copy(t, side).start()

    def take(t):
        pair = t // NC
        c = t - pair * NC
        acc = product(pair, 0, c)
        for side in range(2):
            pair_copy(t, side).wait_recv()
            rows = part(2 * pair + side, 0, blk)
            both = acc[side * blk:(side + 1) * blk] + out[rows, col(c)].astype(jnp.float32)
            out[rows, col(c)] = both.astype(jnp.bfloat16)

            @pl.when(pair == 0)
            def _():
                far_copy(c, side).start()

            @pl.when(jnp.logical_and(pair == 1, c == NC - 1))
            def _():
                near_copy(side).start()

    def first_pair(i, side):
        at, size = pieces[i]
        return remote(
            stage.at[0, pl.ds(side * blk, blk), pl.ds(at, size)],
            out.at[pl.ds(part_row(side, chip, 1 - core), blk), pl.ds(at, size)],
            pair_s.at[4 * i, side], pair_r.at[i * steps, side], sib,
        )

    def first_far(i, side):
        at, size = pieces[i]
        to = chip_at(1 - 2 * side)
        return remote(
            out.at[part(side, 0, blk), pl.ds(at, size)],
            out.at[pl.ds(recv_row(side, to, core), blk), pl.ds(at, size)],
            rs_s.at[side, i * (NC + 1)], rs_r.at[side, i * (NC + 1)], 2 * to + core,
        )

    def first_product(i, which):
        at, size = pieces[i]
        return jnp.dot(
            xbuf[0, which], wbuf[0, :, at:at + size], preferred_element_type=jnp.float32
        )

    def first_give(i):
        at, size = pieces[i]
        stage[0, :, at:at + size] = first_product(i, 1).astype(jnp.bfloat16)

    def first_take(i, acc):
        at, size = pieces[i]
        for side in range(2):
            first_pair(i, side).wait_recv()
            rows = part(side, 0, blk)
            there = out[rows, at:at + size].astype(jnp.float32)
            out[rows, at:at + size] = (acc[side * blk:(side + 1) * blk] + there).astype(jnp.bfloat16)
            first_far(i, side).start()

    wait_x(0, 1)
    load_w0(0).wait()
    first_give(0)
    pl.semaphore_wait(barrier, 3)
    for side in range(2):
        first_pair(0, side).start()
    wait_x(0, 0)
    first_take(0, first_product(0, 0))
    load_w0(1).wait()
    load_w(2).start()
    first_give(1)
    for side in range(2):
        first_pair(1, side).start()
    first_take(1, first_product(1, 0))
    for i in range(2):
        for side in range(2):
            first_pair(i, side).wait_send()

    @pl.loop(1, steps + 1)
    def _(t):
        @pl.when(t < steps)
        def _():
            pair = t // NC
            c = t - pair * NC

            @pl.when(c == 0)
            def _():
                wait_x(pair, 1)

            @pl.when(t < NC)
            def _():
                load_w(c).wait()

            @pl.when(t < NC - 2)
            def _():
                load_w(c + 2).start()

            @pl.when(t == NC // 2)
            def _():
                start_x(1, 1)
                start_x(1, 0)
                load_r.start()
                load_g.start()

            @pl.when(t > 4)
            def _():
                for side in range(2):
                    pair_copy(t - 4, side).wait_send()

            give(t)
            start_give(t)

        @pl.when(t > 1)
        def _():
            u = t - 1
            pair = u // NC
            c = u - pair * NC

            @pl.when(c == 0)
            def _():
                wait_x(pair, 0)

            take(u)

            @pl.when(jnp.logical_and(c == NC - 1, pair < 2))
            def _():
                start_x(pair + 2, 1)
                start_x(pair + 2, 0)

    def cb_copy(i):
        s = i // 2
        side = i - 2 * s
        to = chip_at(1 - 2 * side)
        dst = pl.multiple_of(recv_row(4 + side, to, core) + s * sub, sub)
        return remote(
            out.at[part(4 + side, s * sub, sub), :], out.at[pl.ds(dst, sub), :],
            cb_s.at[i], cb_r.at[i], 2 * to + core,
        )

    for i in range(2):
        for side in range(2):
            first_far(i, side).wait_recv()

    @pl.loop(1, NC)
    def _(c):
        for side in range(2):
            far_copy(c, side).wait_recv()

    @pl.loop(0, 2 * NS)
    def _(i):
        s = i // 2
        side = i - 2 * s
        total = out[part(4 + side, s * sub, sub), :].astype(jnp.float32)
        total = total + out[recv(side, s * sub, sub), :].astype(jnp.float32)
        out[part(4 + side, s * sub, sub), :] = total.astype(jnp.bfloat16)
        cb_copy(i).start()

    def tell_ready(which):
        for dev in (sib, left, right):
            pl.semaphore_signal(
                ready.at[which], inc=1, device_id={"tp": dev}, device_id_type=MESH
            )

    for i in range(2):
        for side in range(2):
            first_far(i, side).wait_send()

    @pl.loop(1, NC)
    def _(c):
        for side in range(2):
            far_copy(c, side).wait_send()

    for side in range(2):
        near_copy(side).wait_send()

    @pl.loop(steps - 4, steps)
    def _(t):
        for side in range(2):
            pair_copy(t, side).wait_send()

    tell_ready(0)

    for side in range(2):
        near_copy(side).wait_recv()

    load_r.wait()
    load_g.wait()
    pl.semaphore_wait(ready.at[0], 3)

    def two_chunks(q, i):
        half = i // 2
        row = row_of(q, core, i - 2 * half) + half * 2 * sub
        return out.at[pl.ds(pl.multiple_of(row, 2 * sub), 2 * sub), :]

    def ag_copy(i, d):
        rows = two_chunks(chip, i)
        return remote(rows, rows, ag_s.at[d, i], ag_r.at[d, i], right if d == 0 else left)

    def own_sib(i):
        rows = two_chunks(chip, i)
        return remote(rows, rows, sib_s.at[0, i], sib_r.at[0, i], sib)

    grp = 16 if sub % 16 == 0 else sub

    @pl.loop(0, 2 * NS)
    def _(i):
        s = i // 2
        o = i - 2 * s
        cb_copy(2 * s + 1 - o).wait_recv()

        @pl.loop(0, sub // grp)
        def _(b):
            at = s * sub + b * grp
            y = out[part(6 + o, at, grp), :].astype(jnp.float32)
            y = y + out[recv(2 + o, at, grp), :].astype(jnp.float32)
            y = y + out[recv(5 - o, at, grp), :].astype(jnp.float32)
            rr = rbuf[pl.ds(pl.multiple_of(o * blk + at, grp), grp), :]
            a = rr.astype(jnp.float32) + y.astype(jnp.bfloat16).astype(jnp.float32)
            ms = jnp.mean(a * a, axis=-1, keepdims=True)
            z = a * lax.rsqrt(ms + EPS) * gbuf[...].astype(jnp.float32).reshape(1, -1)
            out[part(6 + o, at, grp), :] = z.astype(jnp.bfloat16)

        @pl.when(s - 2 * (s // 2) == 1)
        def _():
            done = s - 1 + o
            ag_copy(done, 0).start()
            ag_copy(done, 1).start()
            own_sib(done).start()

    @pl.loop(0, 2 * NS)
    def _(i):
        cb_copy(i).wait_send()

    tell_ready(1)
    pl.semaphore_wait(ready.at[1], 3)

    def sib_copy(d, i):
        rows = two_chunks(chip_at(-1 if d == 0 else 1), i)
        return remote(rows, rows, sib_s.at[1 + d, i], sib_r.at[1 + d, i], sib)

    tail = [(s * sub, sub) for s in range(NS - 1)]
    tail += [(blk - sub, sub // 2), (blk - sub // 2, sub // 4)]
    tail += [(blk - sub // 4, sub // 8), (blk - sub // 8, sub // 8)]

    def fw_rows(q, d, p):
        at, size = tail[p]
        return out.at[pl.ds(pl.multiple_of(row_of(q, core, d) + at, size), size), :]

    def fw_copy(d, p):
        rows = fw_rows(chip_at(-1 if d == 0 else 1), d, p)
        return remote(rows, rows, fw_s.at[d, p], fw_r.at[d, p], right if d == 0 else left)

    def fw_in(d, p):
        rows = fw_rows(chip_at(2), d, p)
        return remote(rows, rows, fw_s.at[d, p], fw_r.at[d, p], sib)

    def fw_sib(d, p):
        rows = fw_rows(chip_at(2), d, p)
        return remote(rows, rows, ts_s.at[d, p], ts_r.at[d, p], sib)

    for half in range(NS // 2):
        for o in range(2):
            i = 2 * half + o
            for d in range(2):
                ag_copy(i, d).wait_recv()
                if o == d:
                    for p in range(2 * half, len(tail) if half else 2):
                        fw_copy(d, p).start()
                sib_copy(d, i).start()

    @pl.loop(0, NS)
    def _(i):
        own_sib(i).wait()
        for d in range(2):
            ag_copy(i, d).wait_send()
            sib_copy(d, i).wait()

    for p in range(len(tail)):
        for d in range(2):
            fw_in(d, p).wait_recv()
            fw_sib(d, p).start()
            fw_copy(d, p).wait_send()
            if p:
                fw_sib(d, p - 1).wait()

    for d in range(2):
        fw_sib(d, len(tail) - 1).wait()


def write_out(z, o, sem):
    rows = z.shape[0] // sem.shape[0]
    copies = [
        pltpu.make_async_copy(z.at[pl.ds(i * rows, rows), :], o.at[pl.ds(i * rows, rows), :], sem.at[i])
        for i in range(sem.shape[0])
    ]
    for cp in copies:
        cp.start()
    for cp in copies:
        cp.wait()


def solution(mesh):
    tp = mesh.shape["tp"]

    def local(x, w, r, g):
        t, f = x.shape
        h = w.shape[1]
        blk = t // (2 * tp)
        dma = pltpu.SemaphoreType.DMA
        bf16 = jnp.bfloat16
        any_spec = pl.BlockSpec(memory_space=pl.ANY)
        z = pl.pallas_call(
            functools.partial(kernel, tp),
            out_shape=pltpu.VMEM((t, h), bf16),
            in_specs=[any_spec] * 4,
            out_specs=pl.BlockSpec(memory_space=pltpu.VMEM),
            scratch_shapes=[
                pltpu.VMEM((2, 2, 2 * blk, f), bf16),
                pltpu.VMEM((NC, f, h // NC), bf16),
                pltpu.VMEM((h,), bf16),
                pltpu.VMEM((2 * blk, h), bf16),
                pltpu.VMEM((4, 2 * blk, h // NC), bf16),
                dma((2, 2, 2)), dma((NC + 1,)), dma((2,)),
                dma((5, 2)), dma((4 * NC + 1, 2)),
                dma((2, NC + 2)), dma((2, NC + 2)),
                dma((2 * NS,)), dma((2 * NS,)),
                dma((2, NS)), dma((2, NS)),
                dma((2, NS + 3)), dma((2, NS + 3)),
                dma((2, NS + 3)), dma((2, NS + 3)),
                dma((3, NS)), dma((3, NS)),
                pltpu.SemaphoreType.REGULAR((2,)),
            ],
            compiler_params=pltpu.CompilerParams(
                collective_id=0, has_side_effects=True, vmem_limit_bytes=VMEM_COMM,
            ),
            cost_estimate=pl.CostEstimate(
                flops=2 * t * f * h, bytes_accessed=2 * (t * f + f * h + 2 * t * h), transcendentals=0
            ),
        )(x, w, r, g)
        return pl.pallas_call(
            write_out,
            out_shape=jax.ShapeDtypeStruct((t, h), bf16),
            in_specs=[pl.BlockSpec(memory_space=pltpu.VMEM)],
            out_specs=any_spec,
            scratch_shapes=[dma((16,))],
            compiler_params=pltpu.CompilerParams(vmem_limit_bytes=VMEM_WRITE),
        )(z)

    return jax.shard_map(
        local,
        mesh=mesh,
        in_specs=(P("data", "tp"), P("tp", None), P("data", None), P(None)),
        out_specs=P("data", None),
        check_vma=False,
    )
```
